8 devices in a mesh: data: 8 (over z, y, x, core).
Axes of the slice: x: 2, y: 2, z: 1, core: 2. Of those that a mesh axis runs over, the one named last changes fastest.
Arguments:
- feat_img: bfloat16 [16384, 768], P('data')
- feat_txt: bfloat16 [16384, 512], P('data')
- w_img: bfloat16 [768, 512], replicated
- w_txt: bfloat16 [512, 512], replicated
- log_temp: float32 [], replicated
- logit_bias: float32 [], replicated
- pair_ids: int32 [16384], P('data')
Outputs:
- output 1: float32 [], replicated
- output 2: float32 [], replicated
- output 3: float32 [], replicated
- output 4: float32 [768, 512], replicated
- output 5: float32 [512, 512], replicated
All inputs are finite; a program needn't handle non-finite values.
Results may differ from the reference program's by a relative error of at most 0.001.
Values are sent between devices in bfloat16 or wider.
A program may use at most 1 GiB of HBM per device.

```python
import jax
import jax.numpy as jnp
from jax import lax

ROWS_DEV = 2048
DEVICES = 8
EMBED = 512
FEAT_IMG = 768
FEAT_TXT = 512
LATENT = 16

BATCH = ROWS_DEV * DEVICES


def feature_draw(base_key, feat_width):
    key_list = jax.random.split(base_key, 4)
    latents = jax.random.normal(key_list[0], (BATCH, LATENT), jnp.float32)
    basis_rows = jax.random.normal(key_list[1], (LATENT, feat_width), jnp.float32)
    center = jax.random.normal(key_list[2], (feat_width,), jnp.float32)
    noise_rows = jax.random.normal(key_list[3], (BATCH, feat_width), jnp.float32)
    feat_out = center + jnp.dot(latents, basis_rows) * LATENT ** -0.5 + 0.5 * noise_rows
    return feat_out.astype(jnp.bfloat16)


def setup_inputs(seed: int = 0) -> dict:
    key_list = jax.random.split(jax.random.key(seed), 7)
    w_img = jax.random.normal(key_list[2], (FEAT_IMG, EMBED), jnp.float32) * FEAT_IMG ** -0.5
    w_txt = jax.random.normal(key_list[3], (FEAT_TXT, EMBED), jnp.float32) * FEAT_TXT ** -0.5
    log_temp = jnp.log(10.0) + jax.random.uniform(key_list[4], (), jnp.float32, -0.5, 0.5)
    logit_bias = -jnp.log(float(BATCH)) + jax.random.uniform(key_list[5], (), jnp.float32, -0.5, 1.5)
    pair_ids = (jax.random.permutation(key_list[6], BATCH) // 2).astype(jnp.int32)
    return {
        "feat_img": feature_draw(key_list[0], FEAT_IMG),
        "feat_txt": feature_draw(key_list[1], FEAT_TXT),
        "w_img": w_img.astype(jnp.bfloat16),
        "w_txt": w_txt.astype(jnp.bfloat16),
        "log_temp": log_temp.astype(jnp.float32),
        "logit_bias": logit_bias.astype(jnp.float32),
        "pair_ids": pair_ids,
    }


def reference(feat_img, feat_txt, w_img, w_txt, log_temp, logit_bias, pair_ids):
    temp_scale = jnp.exp(log_temp)
    raw_img = jnp.dot(feat_img, w_img, preferred_element_type=jnp.float32)
    raw_txt = jnp.dot(feat_txt, w_txt, preferred_element_type=jnp.float32)
    inv_img = lax.rsqrt(jnp.sum(raw_img * raw_img, axis=1, keepdims=True))
    inv_txt = lax.rsqrt(jnp.sum(raw_txt * raw_txt, axis=1, keepdims=True))
    unit_img = raw_img * inv_img
    unit_txt = raw_txt * inv_txt
    emb_img = unit_img.astype(jnp.bfloat16)
    emb_txt = unit_txt.astype(jnp.bfloat16)

    def row_block(loop_state, block_in):
        acc_txt, loss_sum, temp_sum, bias_sum = loop_state
        emb_blk, ids_blk = block_in
        sim_tile = jnp.dot(emb_blk, emb_txt.T, preferred_element_type=jnp.float32)
        label_sign = jnp.where(ids_blk[:, None] == pair_ids[None, :], 1.0, -1.0).astype(jnp.float32)
        margin = -label_sign * (temp_scale * sim_tile + logit_bias)
        grad_tile = -label_sign * jax.nn.sigmoid(margin) / BATCH
        grad_bf = grad_tile.astype(jnp.bfloat16)
        grad_blk = jnp.dot(grad_bf, emb_txt, preferred_element_type=jnp.float32)
        acc_txt = acc_txt + jnp.dot(grad_bf.T, emb_blk, preferred_element_type=jnp.float32)
        new_state = (
            acc_txt,
            loss_sum + jnp.sum(jax.nn.softplus(margin)),
            temp_sum + jnp.sum(grad_tile * sim_tile),
            bias_sum + jnp.sum(grad_tile),
        )
        return new_state, grad_blk

    zero_sum = jnp.zeros((), jnp.float32)
    init_state = (jnp.zeros((BATCH, EMBED), jnp.float32), zero_sum, zero_sum, zero_sum)
    block_in = (emb_img.reshape(DEVICES, ROWS_DEV, EMBED), pair_ids.reshape(DEVICES, ROWS_DEV))
    final_state, grad_blocks = lax.scan(row_block, init_state, block_in)
    acc_txt, loss_sum, temp_sum, bias_sum = final_state
    grad_img = temp_scale * grad_blocks.reshape(BATCH, EMBED)
    grad_txt = temp_scale * acc_txt
    raw_grad_img = inv_img * (grad_img - unit_img * jnp.sum(unit_img * grad_img, axis=1, keepdims=True))
    raw_grad_txt = inv_txt * (grad_txt - unit_txt * jnp.sum(unit_txt * grad_txt, axis=1, keepdims=True))
    grad_w_img = jnp.dot(feat_img.T, raw_grad_img.astype(jnp.bfloat16), preferred_element_type=jnp.float32)
    grad_w_txt = jnp.dot(feat_txt.T, raw_grad_txt.astype(jnp.bfloat16), preferred_element_type=jnp.float32)
    return loss_sum / BATCH, temp_scale * temp_sum, bias_sum, grad_w_img, grad_w_txt
```

```python
import functools

import jax
import jax.numpy as jnp
from jax import lax
from jax.experimental import pallas as pl
from jax.experimental.pallas import tpu as pltpu
from jax.sharding import PartitionSpec as P

CONTRACT_ROWS = (((0,), (0,)), ((), ()))
CONTRACT_COLS = (((1,), (1,)), ((), ()))
F32 = jnp.float32
BF16 = jnp.bfloat16
MESH = pl.DeviceIdType.MESH
LOG2E = 1.4426950408889634
N_DEV = 8
ROW_BLK = 512
COL_BLK = 1024
STRIP = 64

REL_P, REL_X, REL_Y, REL_XP, REL_YP, REL_D, REL_DP = range(7)


def flip_bits(core, cx, cy, fc, fx, fy):
    return (core + fc - 2 * core * fc) + 2 * (cx + fx - 2 * cx * fx) + 4 * (cy + fy - 2 * cy * fy)


def enter(me, peers):
    barrier = pltpu.get_barrier_semaphore()
    for peer in peers:
        pl.semaphore_signal(barrier, inc=1, device_id=(peer,), device_id_type=MESH)
    pl.semaphore_wait(barrier, len(peers))


def embed_kernel(x_img, x_txt, w_img, w_txt, e_img, e_txt):
    for x, w, e in ((x_img, w_img, e_img), (x_txt, w_txt, e_txt)):
        raw = jnp.dot(x[...], w[...], preferred_element_type=F32)
        inv = lax.rsqrt(jnp.sum(raw * raw, axis=1, keepdims=True))
        e[...] = (raw * inv).astype(BF16)


def embed(feat_img, feat_txt, w_img, w_txt):
    rows, blk = feat_img.shape[0], 512
    width = w_img.shape[1]
    by_row = lambda n: pl.BlockSpec((blk, n), lambda i: (i, 0))
    whole = lambda w: pl.BlockSpec(w.shape, lambda i: (0, 0))
    return pl.pallas_call(
        embed_kernel, name="embed", grid=(rows // blk,),
        out_shape=(jax.ShapeDtypeStruct((rows, width), BF16), jax.ShapeDtypeStruct((rows, width), BF16)),
        in_specs=[by_row(feat_img.shape[1]), by_row(feat_txt.shape[1]), whole(w_img), whole(w_txt)],
        out_specs=(by_row(width), by_row(width)),
    )(feat_img, feat_txt, w_img, w_txt)


def weight_kernel(scale, x_img, x_txt, w_img, w_txt, d_img, d_txt, sums, dw, part):
    first = pl.program_id(0) == 0
    n_img = x_img.shape[1]

    @pl.when(first)
    def _():
        dw[...] = jnp.zeros_like(dw)
        for k in range(4):
            total = sums[k, :, 0:128]
            for j in range(1, sums.shape[2] // 128):
                total = total + sums[k, :, j * 128:(j + 1) * 128]
            part[:, k * 128:(k + 1) * 128] = total

    for x, w, d, span in ((x_img, w_img, d_img, slice(0, n_img)), (x_txt, w_txt, d_txt, slice(n_img, dw.shape[0]))):
        raw = jnp.dot(x[...], w[...], preferred_element_type=F32)
        inv = lax.rsqrt(jnp.sum(raw * raw, axis=1, keepdims=True))
        unit = raw * inv
        grad = scale[0] * d[...]
        raw_grad = inv * (grad - unit * jnp.sum(unit * grad, axis=1, keepdims=True))
        dw[span, :] += lax.dot_general(x[...], raw_grad.astype(BF16), CONTRACT_ROWS, preferred_element_type=F32)


def weight_grads(scale, feat_img, feat_txt, w_img, w_txt, d_img, d_txt, sums):
    rows, blk = feat_img.shape[0], 512
    width = w_img.shape[1]
    n_all = feat_img.shape[1] + feat_txt.shape[1]
    by_row = lambda n: pl.BlockSpec((blk, n), lambda i: (i, 0))
    whole = lambda shape: pl.BlockSpec(shape, lambda i: (0,) * len(shape))
    return pl.pallas_call(
        weight_kernel, name="weight_grads", grid=(rows // blk,),
        out_shape=(jax.ShapeDtypeStruct((n_all, width), F32), jax.ShapeDtypeStruct((8, 512), F32)),
        in_specs=[pl.BlockSpec(memory_space=pltpu.SMEM), by_row(feat_img.shape[1]), by_row(feat_txt.shape[1]),
                  whole(w_img.shape), whole(w_txt.shape), by_row(width), by_row(width), whole(sums.shape)],
        out_specs=(whole((n_all, width)), whole((8, 512))),
    )(scale, feat_img, feat_txt, w_img, w_txt, d_img, d_txt, sums)


def reduce_kernel(x, part, out, total, acc, got, got_a, got_b, got_a2, got_b2, parts, send_sem, recv_sem, p_send, p_recv):
    me = lax.axis_index("data")
    core, cx, cy = me % 2, (me // 2) % 2, me // 4
    partner = flip_bits(core, cx, cy, 1, 0, 0)
    xn, yn = flip_bits(core, cx, cy, 0, 1, 0), flip_bits(core, cx, cy, 0, 0, 1)
    peers = [flip_bits(core, cx, cy, k % 2, (k // 2) % 2, k // 4) for k in range(1, 8)]
    enter(me, peers)
    half = x.shape[0] // 2
    quarter = half // 4
    eighth = quarter // 2

    def rows(start, size):
        return pl.ds(pl.multiple_of(start, 8), size)

    def copy(src, dst, k, to):
        return pltpu.make_async_remote_copy(src_ref=src, dst_ref=dst, send_sem=send_sem.at[k], recv_sem=recv_sem.at[k],
                                            device_id=(to,), device_id_type=MESH)

    def both(one, two):
        one.start()
        two.start()
        one.wait()
        two.wait()

    fold_halves = copy(x.at[rows((1 - core) * half, half)], got, 0, partner)
    fold_halves.start()
    part_copies = [
        pltpu.make_async_remote_copy(src_ref=part, dst_ref=parts.at[me], send_sem=p_send.at[k], recv_sem=p_recv.at[k],
                                     device_id=(peers[k],), device_id_type=MESH) for k in range(7)]
    for cp in part_copies:
        cp.start()
    parts[pl.ds(me, 1)] = part[...][None]
    fold_halves.wait()
    acc[...] = x[rows(core * half, half), :] + got[...]
    a1, b1 = cx * quarter, 2 * quarter + cy * quarter
    both(copy(acc.at[rows((1 - cx) * quarter, quarter)], got_a, 1, xn),
         copy(acc.at[rows(2 * quarter + (1 - cy) * quarter, quarter)], got_b, 2, yn))
    acc[rows(a1, quarter), :] += got_a[...]
    acc[rows(b1, quarter), :] += got_b[...]
    a2, b2 = a1 + cy * eighth, b1 + cx * eighth
    both(copy(acc.at[rows(a1 + (1 - cy) * eighth, eighth)], got_a2, 3, yn),
         copy(acc.at[rows(b1 + (1 - cx) * eighth, eighth)], got_b2, 4, xn))
    base = core * half
    out[rows(base + a2, eighth), :] = acc[rows(a2, eighth), :] + got_a2[...]
    out[rows(base + b2, eighth), :] = acc[rows(b2, eighth), :] + got_b2[...]

    def spread(start, size, k, to):
        span = rows(base + start, size)
        return copy(out.at[span], out.at[span], k, to)

    both(spread(a2, eighth, 5, yn), spread(b2, eighth, 6, xn))
    both(spread(a1, quarter, 7, xn), spread(b1, quarter, 8, yn))
    last = spread(0, half, 9, partner)
    last.start()
    for cp in part_copies:
        cp.wait()
    sum_parts = parts[0]
    for k in range(1, N_DEV):
        sum_parts = sum_parts + parts[k]
    total[...] = sum_parts
    last.wait()


def all_reduce(x, part):
    half, width = x.shape[0] // 2, x.shape[1]
    vmem = pl.BlockSpec(memory_space=pltpu.VMEM)
    buf = lambda n: pltpu.VMEM((n, width), F32)
    return pl.pallas_call(
        reduce_kernel, name="all_reduce",
        out_shape=(jax.ShapeDtypeStruct(x.shape, F32), jax.ShapeDtypeStruct(part.shape, F32)),
        in_specs=[vmem, vmem], out_specs=(vmem, vmem),
        scratch_shapes=[buf(half), buf(half), buf(half // 4), buf(half // 4), buf(half // 8), buf(half // 8),
                        pltpu.VMEM((N_DEV,) + part.shape, F32),
                        pltpu.SemaphoreType.DMA((10,)), pltpu.SemaphoreType.DMA((10,)),
                        pltpu.SemaphoreType.DMA((7,)), pltpu.SemaphoreType.DMA((7,))],
        compiler_params=pltpu.CompilerParams(collective_id=1, has_side_effects=True),
    )(x, part)


def pair_kernel(coef, emb_img, emb_txt, ids_row, ids_col, d_img, d_txt, sums,
                all_img, all_txt, all_ids, sb_img, sb_txt, gb_img, gb_txt, send_sem, recv_sem, id_send, id_recv, own_sem):
    me = lax.axis_index("data")
    core, cx, cy = me % 2, (me // 2) % 2, me // 4
    rows = emb_img.shape[0]
    half = rows // 2

    flip = functools.partial(flip_bits, core, cx, cy)
    flips = {REL_P: (1, 0, 0), REL_X: (0, 1, 0), REL_Y: (0, 0, 1), REL_XP: (1, 1, 0), REL_YP: (1, 0, 1),
             REL_D: (0, 1, 1), REL_DP: (1, 1, 1)}
    dev = {rel: flip(*bits) for rel, bits in flips.items()}

    enter(me, [dev[rel] for rel in range(7)])

    gathered = (all_txt, all_img)
    own = (emb_txt, emb_img)

    def copy_of(feat, hf, src_rel, to_rel, land_rel):
        span = pl.ds(hf * half, half)
        if src_rel is None:
            src, at = own[feat].at[span], me
        else:
            src, at = gathered[feat].at[dev[src_rel], span], dev[src_rel]
        return pltpu.make_async_remote_copy(
            src_ref=src, dst_ref=gathered[feat].at[at, span],
            send_sem=send_sem.at[feat, land_rel, hf], recv_sem=recv_sem.at[feat, land_rel, hf],
            device_id=(dev[to_rel],), device_id_type=MESH)

    T, I = 0, 1
    sends = []

    def send(feat, hf, src_rel, to_rel, land_rel):
        cp = copy_of(feat, hf, src_rel, to_rel, land_rel)
        cp.start()
        sends.append((feat, hf, src_rel, to_rel, land_rel))

    def arrive(feat, hf, rel):
        span = pl.ds(hf * half, half)
        pltpu.make_async_remote_copy(
            src_ref=own[feat].at[span], dst_ref=gathered[feat].at[dev[rel], span],
            send_sem=send_sem.at[feat, rel, hf], recv_sem=recv_sem.at[feat, rel, hf],
            device_id=(dev[REL_P],), device_id_type=MESH).wait_recv()

    id_copies = []
    for rel in range(7):
        cp = pltpu.make_async_remote_copy(
            src_ref=ids_col, dst_ref=all_ids.at[me], send_sem=id_send.at[rel], recv_sem=id_recv.at[rel],
            device_id=(dev[rel],), device_id_type=MESH)
        cp.start()
        id_copies.append(cp)
    for hf in range(2):
        send(T, hf, None, REL_X, REL_X)
        send(I, hf, None, REL_Y, REL_Y)
        send(I, hf, None, REL_X, REL_X)
        send(T, hf, None, REL_Y, REL_Y)
        send(T, hf, None, REL_P, REL_P)
        send(I, hf, None, REL_P, REL_P)
    locals_ = [pltpu.make_async_copy(emb_txt, all_txt.at[me], own_sem.at[0]),
               pltpu.make_async_copy(emb_img, all_img.at[me], own_sem.at[1]),
               pltpu.make_async_copy(ids_col, all_ids.at[me], own_sem.at[2])]
    for cp in locals_:
        cp.start()
    d_img[...] = jnp.zeros_like(d_img)
    d_txt[...] = jnp.zeros_like(d_txt)
    sums[...] = jnp.zeros_like(sums)
    for cp in locals_:
        cp.wait()

    a, b = coef[0], coef[1]
    n_row = rows // ROW_BLK
    n_col = rows // COL_BLK
    n_flat = N_DEV * n_col * n_row

    def where_at(step):
        g, q, e = step // 4, (step % 4) // 2, step % 2
        m0, m3, m2 = (3 - g) // 3, g // 3, (g % 3) // 2
        m12 = 1 - m0 - m3
        fc = m0 * q + (1 - m0) * e
        txt = flip(fc, m12 * (1 - q) + m3, m12 * q + m3)
        img = flip(fc, m12 * q + m3, m12 * (1 - q) + m3)
        return txt, m0 * e + m2 + m3 * (1 - q), img, m0 * e + m2 + m3 * q

    def scores(own_all, r0, other_all, at, hf):
        c0 = pl.multiple_of(hf * COL_BLK, COL_BLK)
        return lax.dot_general(own_all[me, pl.ds(r0, ROW_BLK), :], other_all[at, pl.ds(c0, COL_BLK), :], CONTRACT_COLS,
                               preferred_element_type=F32)

    def sign_of(r0, k, at, hf):
        ids_c = all_ids[at, :, pl.ds(pl.multiple_of(hf * COL_BLK, COL_BLK), COL_BLK)]
        ids_r = ids_row[pl.ds(r0 + k * STRIP, STRIP), 0:1]
        return jnp.where(ids_r == ids_c, -1.0, 1.0).astype(F32)

    def full_tile(r0, at, hf):
        run, low, gs_sum, g_sum = None, None, None, None
        for k in range(ROW_BLK // STRIP):
            s = sb_img[k * STRIP:(k + 1) * STRIP, :]
            sign = sign_of(r0, k, at, hf)
            neg = (s * a + b) * sign
            w = jnp.exp2(-jnp.abs(neg))
            d = 1.0 + w
            g = sign / (1.0 + jnp.exp2(neg))
            low_k, gs = jnp.minimum(neg, 0.0), g * s
            for u in range(STRIP // 8):
                at8 = slice(u * 8, u * 8 + 8)
                run = w[at8] if run is None else run * d[at8] + w[at8]
                low = low_k[at8] if low is None else low + low_k[at8]
                gs_sum = gs[at8] if gs_sum is None else gs_sum + gs[at8]
                g_sum = g[at8] if g_sum is None else g_sum + g[at8]
            gb_img[k * STRIP:(k + 1) * STRIP, :] = g.astype(BF16)
        sums[0] += low
        sums[1] += jnp.log1p(run)
        sums[2] += gs_sum
        sums[3] += g_sum

    def grad_tile(r0, at, hf):
        for k in range(ROW_BLK // STRIP):
            s = sb_txt[k * STRIP:(k + 1) * STRIP, :]
            sign = sign_of(r0, k, at, hf)
            gb_txt[k * STRIP:(k + 1) * STRIP, :] = (sign / (1.0 + jnp.exp2((s * a + b) * sign))).astype(BF16)

    sb_img[...] = scores(all_img, 0, all_txt, me, 0)

    @pl.loop(0, n_flat // n_row)
    def _(step):
        def on(s, arrivals, forwards=(), ids=False):
            @pl.when(step == s)
            def _():
                if ids:
                    for cp in id_copies:
                        cp.wait_recv()
                for item in arrivals:
                    arrive(*item)
                for item in forwards:
                    send(*item)

        on(1, [(T, 0, REL_P), (I, 0, REL_P)], ids=True)
        on(2, [(T, 1, REL_P), (I, 1, REL_P)])
        on(3, [(T, 0, REL_X), (I, 0, REL_Y)],
           [(T, 0, REL_X, REL_P, REL_XP), (I, 0, REL_Y, REL_P, REL_YP), (I, 0, REL_Y, REL_X, REL_D)])
        on(4, [(T, 0, REL_XP), (I, 0, REL_YP)])
        on(5, [(T, 0, REL_Y), (I, 0, REL_X)],
           [(T, 0, REL_Y, REL_P, REL_YP), (I, 0, REL_X, REL_P, REL_XP), (T, 0, REL_Y, REL_X, REL_D)])
        on(6, [(T, 0, REL_YP), (I, 0, REL_XP)])
        on(7, [(T, 1, REL_X), (I, 1, REL_Y)],
           [(T, 1, REL_X, REL_P, REL_XP), (I, 1, REL_Y, REL_P, REL_YP), (T, 1, REL_X, REL_Y, REL_D)])
        on(8, [(T, 1, REL_XP), (I, 1, REL_YP)])
        on(9, [(T, 1, REL_Y), (I, 1, REL_X)],
           [(T, 1, REL_Y, REL_P, REL_YP), (I, 1, REL_X, REL_P, REL_XP), (I, 1, REL_X, REL_Y, REL_D)])
        on(10, [(T, 1, REL_YP), (I, 1, REL_XP)])
        on(11, [(T, 1, REL_D), (I, 0, REL_D)], [(T, 1, REL_D, REL_P, REL_DP), (I, 0, REL_D, REL_P, REL_DP)])
        on(12, [(T, 1, REL_DP), (I, 0, REL_DP)])
        on(13, [(T, 0, REL_D), (I, 1, REL_D)], [(T, 0, REL_D, REL_P, REL_DP), (I, 1, REL_D, REL_P, REL_DP)])
        on(14, [(T, 0, REL_DP), (I, 1, REL_DP)])

        at_t, h_t, at_i, h_i = where_at(step)
        c_t = pl.multiple_of(h_t * COL_BLK, COL_BLK)
        c_i = pl.multiple_of(h_i * COL_BLK, COL_BLK)

        @pl.loop(0, n_row)
        def _(i):
            after = (step * n_row + i + 1) % n_flat
            at_n, h_n, _, _ = where_at(after // n_row)
            r0 = pl.multiple_of(i * ROW_BLK, ROW_BLK)
            r1 = pl.multiple_of((after % n_row) * ROW_BLK, ROW_BLK)
            tile = pl.ds(r0, ROW_BLK)
            sb_txt[...] = scores(all_txt, r0, all_img, at_i, h_i)
            full_tile(r0, at_t, h_t)
            d_img[tile, :] += jnp.dot(gb_img[...], all_txt[at_t, pl.ds(c_t, COL_BLK), :], preferred_element_type=F32)
            sb_img[...] = scores(all_img, r1, all_txt, at_n, h_n)
            grad_tile(r0, at_i, h_i)
            d_txt[tile, :] += jnp.dot(gb_txt[...], all_img[at_i, pl.ds(c_i, COL_BLK), :], preferred_element_type=F32)

    for cp in id_copies:
        cp.wait_send()
    for item in sends:
        copy_of(*item).wait_send()


def pair_grads(coef, emb_img, emb_txt, ids):
    rows, width = emb_img.shape
    vmem = pl.BlockSpec(memory_space=pltpu.VMEM)
    hbm = pl.BlockSpec(memory_space=pl.ANY)
    ids_row = jnp.broadcast_to(ids[:, None], (rows, 128))
    return pl.pallas_call(
        pair_kernel,
        name="pair_grads",
        out_shape=(jax.ShapeDtypeStruct((rows, width), F32), jax.ShapeDtypeStruct((rows, width), F32),
                   jax.ShapeDtypeStruct((4, 8, COL_BLK), F32)),
        in_specs=[pl.BlockSpec(memory_space=pltpu.SMEM), hbm, hbm, vmem, hbm],
        out_specs=(vmem, vmem, vmem),
        scratch_shapes=[
            pltpu.VMEM((N_DEV, rows, width), BF16),
            pltpu.VMEM((N_DEV, rows, width), BF16),
            pltpu.VMEM((N_DEV, 1, rows), jnp.int32),
            pltpu.VMEM((ROW_BLK, COL_BLK), F32),
            pltpu.VMEM((ROW_BLK, COL_BLK), F32),
            pltpu.VMEM((ROW_BLK, COL_BLK), BF16),
            pltpu.VMEM((ROW_BLK, COL_BLK), BF16),
            pltpu.SemaphoreType.DMA((2, 7, 2)),
            pltpu.SemaphoreType.DMA((2, 7, 2)),
            pltpu.SemaphoreType.DMA((7,)),
            pltpu.SemaphoreType.DMA((7,)),
            pltpu.SemaphoreType.DMA((3,)),
        ],
        compiler_params=pltpu.CompilerParams(collective_id=0, has_side_effects=True, vmem_limit_bytes=67_000_000),
    )(coef, emb_img, emb_txt, ids_row, ids[None, :])


def solution(mesh):
    n_dev = mesh.shape["data"]

    def local_fn(feat_img, feat_txt, w_img, w_txt, log_temp, logit_bias, pair_ids):
        total_rows = feat_img.shape[0] * n_dev
        temp_scale = jnp.exp(log_temp)
        emb_img, emb_txt = embed(feat_img, feat_txt, w_img, w_txt)
        coef = jnp.stack([-LOG2E * temp_scale, -LOG2E * logit_bias])
        d_img, d_txt, sums = pair_grads(coef, emb_img, emb_txt, pair_ids)
        scale = temp_scale / total_rows
        dw, part = weight_grads(scale[None], feat_img, feat_txt, w_img, w_txt, d_img, d_txt, sums)
        dw, total = all_reduce(dw, part)
        total = jnp.sum(total.reshape(8, 4, 128), axis=(0, 2))
        n_img = feat_img.shape[1]
        loss = (total[1] - total[0] / LOG2E) / total_rows
        return loss, scale * total[2], total[3] / total_rows, dw[:n_img], dw[n_img:]

    return jax.shard_map(
        local_fn,
        mesh=mesh,
        in_specs=(P("data", None), P("data", None), P(None, None), P(None, None), P(), P(), P("data")),
        out_specs=(P(), P(), P(), P(None, None), P(None, None)),
        check_vma=False,
    )
```

```python
import functools

import jax
import jax.numpy as jnp
from jax import lax
from jax.experimental import pallas as pl
from jax.experimental.pallas import tpu as pltpu
from jax.sharding import PartitionSpec as P

CONTRACT_ROWS = (((0,), (0,)), ((), ()))
CONTRACT_COLS = (((1,), (1,)), ((), ()))
F32 = jnp.float32
BF16 = jnp.bfloat16
MESH = pl.DeviceIdType.MESH
LOG2E = 1.4426950408889634
N_DEV = 8
ROW_BLK = 512
COL_BLK = 1024
STRIP = 64


def flip_bits(core, cx, cy, fc, fx, fy):
    return (core + fc - 2 * core * fc) + 2 * (cx + fx - 2 * cx * fx) + 4 * (cy + fy - 2 * cy * fy)


def enter(me, peers):
    barrier = pltpu.get_barrier_semaphore()
    for peer in peers:
        pl.semaphore_signal(barrier, inc=1, device_id=(peer,), device_id_type=MESH)
    pl.semaphore_wait(barrier, len(peers))


def embed_kernel(x_img, x_txt, w_img, w_txt, e_img, e_txt):
    for x, w, e in ((x_img, w_img, e_img), (x_txt, w_txt, e_txt)):
        raw = jnp.dot(x[...], w[...], preferred_element_type=F32)
        inv = lax.rsqrt(jnp.sum(raw * raw, axis=1, keepdims=True))
        e[...] = (raw * inv).astype(BF16)


def embed(feat_img, feat_txt, w_img, w_txt):
    rows, blk = feat_img.shape[0], 512
    width = w_img.shape[1]
    by_row = lambda n: pl.BlockSpec((blk, n), lambda i: (i, 0))
    whole = lambda w: pl.BlockSpec(w.shape, lambda i: (0, 0))
    return pl.pallas_call(
        embed_kernel, name="embed", grid=(rows // blk,),
        out_shape=(jax.ShapeDtypeStruct((rows, width), BF16), jax.ShapeDtypeStruct((rows, width), BF16)),
        in_specs=[by_row(feat_img.shape[1]), by_row(feat_txt.shape[1]), whole(w_img), whole(w_txt)],
        out_specs=(by_row(width), by_row(width)),
    )(feat_img, feat_txt, w_img, w_txt)


def weight_kernel(scale, x_img, x_txt, w_img, w_txt, d_img, r_x, d_txt, r_p, r_y, sums, dw, part):
    first = pl.program_id(0) == 0
    n_img = x_img.shape[1]

    @pl.when(first)
    def _():
        dw[...] = jnp.zeros_like(dw)
        for k in range(4):
            total = sums[k, :, 0:128]
            for j in range(1, sums.shape[2] // 128):
                total = total + sums[k, :, j * 128:(j + 1) * 128]
            part[:, k * 128:(k + 1) * 128] = total

    for x, w, terms, span in ((x_img, w_img, (d_img, r_x), slice(0, n_img)),
                              (x_txt, w_txt, (d_txt, r_p, r_y), slice(n_img, dw.shape[0]))):
        raw = jnp.dot(x[...], w[...], preferred_element_type=F32)
        inv = lax.rsqrt(jnp.sum(raw * raw, axis=1, keepdims=True))
        unit = raw * inv
        total = terms[0][...]
        for term in terms[1:]:
            total = total + term[...]
        grad = scale[0] * total
        raw_grad = inv * (grad - unit * jnp.sum(unit * grad, axis=1, keepdims=True))
        dw[span, :] += lax.dot_general(x[...], raw_grad.astype(BF16), CONTRACT_ROWS, preferred_element_type=F32)


def weight_grads(scale, feat_img, feat_txt, w_img, w_txt, terms, sums):
    rows, blk = feat_img.shape[0], 512
    width = w_img.shape[1]
    n_all = feat_img.shape[1] + feat_txt.shape[1]
    by_row = lambda n: pl.BlockSpec((blk, n), lambda i: (i, 0))
    whole = lambda shape: pl.BlockSpec(shape, lambda i: (0,) * len(shape))
    return pl.pallas_call(
        weight_kernel, name="weight_grads", grid=(rows // blk,),
        out_shape=(jax.ShapeDtypeStruct((n_all, width), F32), jax.ShapeDtypeStruct((8, 512), F32)),
        in_specs=[pl.BlockSpec(memory_space=pltpu.SMEM), by_row(feat_img.shape[1]), by_row(feat_txt.shape[1]),
                  whole(w_img.shape), whole(w_txt.shape), *[by_row(width)] * len(terms), whole(sums.shape)],
        out_specs=(whole((n_all, width)), whole((8, 512))),
    )(scale, feat_img, feat_txt, w_img, w_txt, *terms, sums)


def reduce_kernel(x, part, out, total, acc, got, got_a, got_b, got_a2, got_b2, parts, send_sem, recv_sem, p_send, p_recv):
    me = lax.axis_index("data")
    core, cx, cy = me % 2, (me // 2) % 2, me // 4
    partner = flip_bits(core, cx, cy, 1, 0, 0)
    xn, yn = flip_bits(core, cx, cy, 0, 1, 0), flip_bits(core, cx, cy, 0, 0, 1)
    peers = [flip_bits(core, cx, cy, k % 2, (k // 2) % 2, k // 4) for k in range(1, 8)]
    enter(me, peers)
    half = x.shape[0] // 2
    quarter = half // 4
    eighth = quarter // 2

    def rows(start, size):
        return pl.ds(pl.multiple_of(start, 8), size)

    def copy(src, dst, k, to):
        return pltpu.make_async_remote_copy(src_ref=src, dst_ref=dst, send_sem=send_sem.at[k], recv_sem=recv_sem.at[k],
                                            device_id=(to,), device_id_type=MESH)

    def both(one, two):
        one.start()
        two.start()
        one.wait()
        two.wait()

    fold_halves = copy(x.at[rows((1 - core) * half, half)], got, 0, partner)
    fold_halves.start()
    part_copies = [
        pltpu.make_async_remote_copy(src_ref=part, dst_ref=parts.at[me], send_sem=p_send.at[k], recv_sem=p_recv.at[k],
                                     device_id=(peers[k],), device_id_type=MESH) for k in range(7)]
    for cp in part_copies:
        cp.start()
    parts[pl.ds(me, 1)] = part[...][None]
    fold_halves.wait()
    acc[...] = x[rows(core * half, half), :] + got[...]
    a1, b1 = cx * quarter, 2 * quarter + cy * quarter
    both(copy(acc.at[rows((1 - cx) * quarter, quarter)], got_a, 1, xn),
         copy(acc.at[rows(2 * quarter + (1 - cy) * quarter, quarter)], got_b, 2, yn))
    acc[rows(a1, quarter), :] += got_a[...]
    acc[rows(b1, quarter), :] += got_b[...]
    a2, b2 = a1 + cy * eighth, b1 + cx * eighth
    both(copy(acc.at[rows(a1 + (1 - cy) * eighth, eighth)], got_a2, 3, yn),
         copy(acc.at[rows(b1 + (1 - cx) * eighth, eighth)], got_b2, 4, xn))
    base = core * half
    out[rows(base + a2, eighth), :] = acc[rows(a2, eighth), :] + got_a2[...]
    out[rows(base + b2, eighth), :] = acc[rows(b2, eighth), :] + got_b2[...]

    def spread(start, size, k, to):
        span = rows(base + start, size)
        return copy(out.at[span], out.at[span], k, to)

    both(spread(a2, eighth, 5, yn), spread(b2, eighth, 6, xn))
    both(spread(a1, quarter, 7, xn), spread(b1, quarter, 8, yn))
    last = spread(0, half, 9, partner)
    last.start()
    for cp in part_copies:
        cp.wait()
    sum_parts = parts[0]
    for k in range(1, N_DEV):
        sum_parts = sum_parts + parts[k]
    total[...] = sum_parts
    last.wait()


def all_reduce(x, part):
    half, width = x.shape[0] // 2, x.shape[1]
    vmem = pl.BlockSpec(memory_space=pltpu.VMEM)
    buf = lambda n: pltpu.VMEM((n, width), F32)
    return pl.pallas_call(
        reduce_kernel, name="all_reduce",
        out_shape=(jax.ShapeDtypeStruct(x.shape, F32), jax.ShapeDtypeStruct(part.shape, F32)),
        in_specs=[vmem, vmem], out_specs=(vmem, vmem),
        scratch_shapes=[buf(half), buf(half), buf(half // 4), buf(half // 4), buf(half // 8), buf(half // 8),
                        pltpu.VMEM((N_DEV,) + part.shape, F32),
                        pltpu.SemaphoreType.DMA((10,)), pltpu.SemaphoreType.DMA((10,)),
                        pltpu.SemaphoreType.DMA((7,)), pltpu.SemaphoreType.DMA((7,))],
        compiler_params=pltpu.CompilerParams(collective_id=1, has_side_effects=True),
    )(x, part)


def tile_at(t):
    def from_(s, n):
        return lax.div(n + 64 - s, 64)

    early = 1 - from_(16, t)
    late = t + 16 * early
    b1, b2, b3 = from_(31, late), from_(44, late), from_(55, late)
    k = b1 + b2 + b3
    u = late - (16 + 15 * b1 + 13 * b2 + 11 * b3)
    v = u - (8 - k)
    is_col = from_(0, v)
    i = (1 - is_col) * (4 + k) + is_col * (v + (k + 1) * from_(4, v))
    j = (1 - is_col) * (u + k * from_(4, u)) + is_col * (4 + k)
    return early * lax.rem(t, 4) + (1 - early) * i, early * lax.div(t, 4) + (1 - early) * j


def pair_kernel(coef, emb_img, emb_txt, ids_sq, ids_half, ids_quarter, d_img, d_txt, r_x, r_p, r_y, sums,
                img, txt, di, dt, comb, ids_row, ids_col, ids_x, sb0, sb1, gb0, gb1, send_sem, recv_sem, own_sem):
    me = lax.axis_index("data")
    core, cx, cy = me % 2, (me // 2) % 2, me // 4
    flip = functools.partial(flip_bits, core, cx, cy)
    partner, xn, yn, yp = flip(1, 0, 0), flip(0, 1, 0), flip(0, 0, 1), flip(1, 0, 1)
    rows = emb_img.shape[0]
    q_rows = rows // 4
    enter(me, [partner, xn, yn, yp])

    def copy(k, src, dst, to):
        return pltpu.make_async_remote_copy(src_ref=src, dst_ref=dst, send_sem=send_sem.at[k], recv_sem=recv_sem.at[k],
                                            device_id=(to,), device_id_type=MESH)

    low, high = pl.ds(0, q_rows), pl.ds(q_rows, q_rows)

    def quarter(q):
        return pl.ds(q * q_rows, q_rows)

    feat_x = [copy(q, emb_img.at[quarter(q)], img.at[pl.ds(rows + q * q_rows, q_rows)], xn) for q in range(4)]
    feat_y = [copy(4 + q, emb_txt.at[quarter(q)], txt.at[4 + q, low], yn) for q in range(4)]
    feat_p = [copy(8 + h, emb_txt.at[pl.ds(h * COL_BLK, COL_BLK)], txt.at[2 + h], partner) for h in range(2)]
    pass_p = [copy(10 + q, txt.at[4 + q, low], txt.at[4 + q, high], partner) for q in range(4)]
    part_x = [copy(14 + q, di.at[pl.ds(rows + q * q_rows, q_rows)], r_x.at[quarter(q)], xn) for q in range(4)]
    part_c = [copy(18 + q, dt.at[4 + q, high], comb.at[q], partner) for q in range(4)]
    part_y = [copy(22 + q, dt.at[4 + q, low], r_y.at[quarter(q)], yn) for q in range(4)]
    part_p = [copy(26 + h, dt.at[2 + h], r_p.at[pl.ds(h * COL_BLK, COL_BLK)], partner) for h in range(2)]
    ids_p = copy(28, ids_half, ids_col.at[pl.ds(2, 2)], partner)
    ids_y = copy(29, ids_quarter, ids_col.at[pl.ds(4, 4), :, low], yn)
    ids_yp = copy(30, ids_quarter, ids_col.at[pl.ds(4, 4), :, high], yp)
    ids_xn = copy(31, ids_sq, ids_x.at[1], xn)
    every = [*feat_x, *feat_y, *feat_p, *pass_p, *part_x, *part_c, *part_y, *part_p, ids_p, ids_y, ids_yp, ids_xn]

    for cp in (ids_xn, ids_p, ids_y, ids_yp):
        cp.start()
    for q in range(4):
        feat_x[q].start()
        feat_y[q].start()
    for cp in feat_p:
        cp.start()
    own = [pltpu.make_async_copy(emb_img, img.at[pl.ds(0, rows)], own_sem.at[0]),
           pltpu.make_async_copy(emb_txt.at[pl.ds(0, COL_BLK)], txt.at[0], own_sem.at[1]),
           pltpu.make_async_copy(emb_txt.at[pl.ds(COL_BLK, COL_BLK)], txt.at[1], own_sem.at[2]),
           pltpu.make_async_copy(ids_half, ids_col.at[pl.ds(0, 2)], own_sem.at[3]),
           pltpu.make_async_copy(ids_sq, ids_x.at[0], own_sem.at[4])]
    for cp in own:
        cp.start()

    @pl.loop(0, 8)
    def _(k):
        di[pl.ds(pl.multiple_of(k * ROW_BLK, ROW_BLK), ROW_BLK), :] = jnp.zeros((ROW_BLK, di.shape[1]), F32)
        dt[k] = jnp.zeros(dt.shape[1:], F32)

    sums[...] = jnp.zeros_like(sums)
    gb1[...] = jnp.zeros_like(gb1)
    for cp in own:
        cp.wait()

    def spread_ids(which):
        columns = ids_x[which].T
        for k in range(rows // 128):
            ids_row[which * rows + k * 128:which * rows + (k + 1) * 128, :] = jnp.broadcast_to(
                columns[:, k:k + 1], (128, 128))

    spread_ids(0)
    a, b = coef[0], coef[1]
    n_tiles = 64

    def row_span(i):
        return pl.ds(pl.multiple_of(i * ROW_BLK, ROW_BLK), ROW_BLK)

    def scores(sb, t):
        i, j = tile_at(t)
        sb[...] = lax.dot_general(img[row_span(i), :], txt[j], CONTRACT_COLS, preferred_element_type=F32)

    def gradients(gb, t):
        i, j = tile_at(t)
        di[row_span(i), :] += jnp.dot(gb[...], txt[j], preferred_element_type=F32)
        dt[j] += lax.dot_general(gb[...], img[row_span(i), :], CONTRACT_ROWS, preferred_element_type=F32)

    def elementwise(sb, gb, t):
        i, j = tile_at(t)
        ids_c = ids_col[j]
        run, low_sum, gs_sum, g_sum = None, None, None, None
        for k in range(ROW_BLK // STRIP):
            s = sb[k * STRIP:(k + 1) * STRIP, :]
            ids_r = ids_row[pl.ds(i * ROW_BLK + k * STRIP, STRIP), 0:1]
            sign = jnp.where(ids_r == ids_c, -1.0, 1.0).astype(F32)
            neg = (s * a + b) * sign
            w = jnp.exp2(-jnp.abs(neg))
            d = 1.0 + w
            g = sign / (1.0 + jnp.exp2(neg))
            low_k, gs = jnp.minimum(neg, 0.0), g * s
            for u in range(STRIP // 8):
                at8 = slice(u * 8, u * 8 + 8)
                run = w[at8] if run is None else run * d[at8] + w[at8]
                low_sum = low_k[at8] if low_sum is None else low_sum + low_k[at8]
                gs_sum = gs[at8] if gs_sum is None else gs_sum + gs[at8]
                g_sum = g[at8] if g_sum is None else g_sum + g[at8]
            gb[k * STRIP:(k + 1) * STRIP, :] = g.astype(BF16)
        sums[0] += low_sum
        sums[1] += jnp.log1p(run)
        sums[2] += gs_sum
        sums[3] += g_sum

    def join(q):
        part_c[q].wait_recv()
        dt[4 + q, 0:q_rows, :] += comb[q]
        part_y[q].start()

    scores(sb0, 0)

    @pl.loop(0, n_tiles // 2)
    def _(f):
        def on(at, arrivals=(), starts=(), then=None):
            @pl.when(f == at)
            def _():
                for cp in arrivals:
                    cp.wait_recv()
                for cp in starts:
                    cp.start()
                if then is not None:
                    then()

        on(3, [*feat_p, ids_p])
        on(7, [feat_x[0], feat_y[0], feat_y[1], ids_y, ids_yp, ids_xn], [pass_p[0], pass_p[1]],
           then=functools.partial(spread_ids, 1))
        on(9, [pass_p[0], pass_p[1], feat_y[2]], [pass_p[2]])
        on(10, [pass_p[2], feat_y[3]], [pass_p[3]])
        on(11, [pass_p[3]])
        on(13, feat_x[1:], [part_x[0]])
        on(16, (), [part_c[0]])
        on(17, then=functools.partial(join, 0))
        on(20, (), [part_x[1]])
        on(23, (), [part_c[1]])
        on(24, then=functools.partial(join, 1))
        on(26, (), [part_x[2]])
        on(28, (), [part_c[2]])
        on(29, then=functools.partial(join, 2))
        on(31, (), [part_x[3], *part_p])

        t = 2 * f
        scores(sb1, t + 1)
        elementwise(sb0, gb0, t)
        gradients(gb1, jnp.maximum(t - 1, 0))
        scores(sb0, lax.rem(t + 2, n_tiles))
        elementwise(sb1, gb1, t + 1)
        gradients(gb0, t)

    gradients(gb1, n_tiles - 1)
    part_c[3].start()
    outs = [pltpu.make_async_copy(di.at[pl.ds(0, rows)], d_img, own_sem.at[0]),
            pltpu.make_async_copy(dt.at[0], d_txt.at[pl.ds(0, COL_BLK)], own_sem.at[1]),
            pltpu.make_async_copy(dt.at[1], d_txt.at[pl.ds(COL_BLK, COL_BLK)], own_sem.at[2])]
    for cp in outs:
        cp.start()
    join(3)
    for cp in outs:
        cp.wait()
    for cp in (*part_x, *part_p, *part_y):
        cp.wait_recv()
    for cp in every:
        cp.wait_send()


def pair_grads(coef, emb_img, emb_txt, ids):
    rows, width = emb_img.shape
    hbm = pl.BlockSpec(memory_space=pl.ANY)
    vmem = pl.BlockSpec(memory_space=pltpu.VMEM)
    grads = jax.ShapeDtypeStruct((rows, width), F32)
    return pl.pallas_call(
        pair_kernel,
        name="pair_grads",
        out_shape=(grads, grads, grads, grads, grads, jax.ShapeDtypeStruct((4, 8, COL_BLK), F32)),
        in_specs=[pl.BlockSpec(memory_space=pltpu.SMEM), hbm, hbm, hbm, hbm, hbm],
        out_specs=(hbm, hbm, hbm, hbm, hbm, vmem),
        scratch_shapes=[
            pltpu.VMEM((2 * rows, width), BF16),
            pltpu.VMEM((8, COL_BLK, width), BF16),
            pltpu.VMEM((2 * rows, width), F32),
            pltpu.VMEM((8, COL_BLK, width), F32),
            pltpu.VMEM((4, rows // 4, width), F32),
            pltpu.VMEM((2 * rows, 128), jnp.int32),
            pltpu.VMEM((8, 1, COL_BLK), jnp.int32),
            pltpu.VMEM((2, rows // 128, 128), jnp.int32),
            pltpu.VMEM((ROW_BLK, COL_BLK), F32),
            pltpu.VMEM((ROW_BLK, COL_BLK), F32),
            pltpu.VMEM((ROW_BLK, COL_BLK), BF16),
            pltpu.VMEM((ROW_BLK, COL_BLK), BF16),
            pltpu.SemaphoreType.DMA((32,)),
            pltpu.SemaphoreType.DMA((32,)),
            pltpu.SemaphoreType.DMA((5,)),
        ],
        compiler_params=pltpu.CompilerParams(collective_id=0, has_side_effects=True, vmem_limit_bytes=67_000_000),
    )(coef, emb_img, emb_txt, ids.reshape(rows // 128, 128), ids.reshape(2, 1, COL_BLK), ids.reshape(4, 1, rows // 4))


def solution(mesh):
    n_dev = mesh.shape["data"]

    def local_fn(feat_img, feat_txt, w_img, w_txt, log_temp, logit_bias, pair_ids):
        total_rows = feat_img.shape[0] * n_dev
        temp_scale = jnp.exp(log_temp)
        emb_img, emb_txt = embed(feat_img, feat_txt, w_img, w_txt)
        coef = jnp.stack([-LOG2E * temp_scale, -LOG2E * logit_bias])
        d_img, d_txt, r_x, r_p, r_y, sums = pair_grads(coef, emb_img, emb_txt, pair_ids)
        scale = temp_scale / total_rows
        dw, part = weight_grads(scale[None], feat_img, feat_txt, w_img, w_txt, (d_img, r_x, d_txt, r_p, r_y), sums)
        dw, total = all_reduce(dw, part)
        total = jnp.sum(total.reshape(8, 4, 128), axis=(0, 2))
        n_img = feat_img.shape[1]
        loss = (total[1] - total[0] / LOG2E) / total_rows
        return loss, scale * total[2], total[3] / total_rows, dw[:n_img], dw[n_img:]

    return jax.shard_map(
        local_fn,
        mesh=mesh,
        in_specs=(P("data", None), P("data", None), P(None, None), P(None, None), P(), P(), P("data")),
        out_specs=(P(), P(), P(), P(None, None), P(None, None)),
        check_vma=False,
    )
```

```python
import functools

import jax
import jax.numpy as jnp
from jax import lax
from jax.experimental import pallas as pl
from jax.experimental.pallas import tpu as pltpu
from jax.sharding import PartitionSpec as P

CONTRACT_ROWS = (((0,), (0,)), ((), ()))
CONTRACT_COLS = (((1,), (1,)), ((), ()))
F32 = jnp.float32
BF16 = jnp.bfloat16
MESH = pl.DeviceIdType.MESH
LOG2E = 1.4426950408889634
N_DEV = 8
ROW_BLK = 512
COL_BLK = 1024
STRIP = 64


def flip_bits(core, cx, cy, fc, fx, fy):
    return (core + fc - 2 * core * fc) + 2 * (cx + fx - 2 * cx * fx) + 4 * (cy + fy - 2 * cy * fy)


def enter(me, peers):
    barrier = pltpu.get_barrier_semaphore()
    for peer in peers:
        pl.semaphore_signal(barrier, inc=1, device_id=(peer,), device_id_type=MESH)
    pl.semaphore_wait(barrier, len(peers))


def embed_kernel(x_img, x_txt, w_img, w_txt, e_img, e_txt):
    for x, w, e in ((x_img, w_img, e_img), (x_txt, w_txt, e_txt)):
        raw = jnp.dot(x[...], w[...], preferred_element_type=F32)
        inv = lax.rsqrt(jnp.sum(raw * raw, axis=1, keepdims=True))
        e[...] = (raw * inv).astype(BF16)


def embed(feat_img, feat_txt, w_img, w_txt):
    rows, blk = feat_img.shape[0], 512
    width = w_img.shape[1]
    by_row = lambda n: pl.BlockSpec((blk, n), lambda i: (i, 0))
    whole = lambda w: pl.BlockSpec(w.shape, lambda i: (0, 0))
    return pl.pallas_call(
        embed_kernel, name="embed", grid=(rows // blk,),
        out_shape=(jax.ShapeDtypeStruct((rows, width), BF16), jax.ShapeDtypeStruct((rows, width), BF16)),
        in_specs=[by_row(feat_img.shape[1]), by_row(feat_txt.shape[1]), whole(w_img), whole(w_txt)],
        out_specs=(by_row(width), by_row(width)),
    )(feat_img, feat_txt, w_img, w_txt)


def weight_kernel(scale, x_img, x_txt, w_img, w_txt, d_img, r_x, d_txt, r_p, r_y, sums, dw, part):
    first = pl.program_id(0) == 0
    n_img = x_img.shape[1]

    @pl.when(first)
    def _():
        dw[...] = jnp.zeros_like(dw)
        for k in range(4):
            total = sums[k, :, 0:128]
            for j in range(1, sums.shape[2] // 128):
                total = total + sums[k, :, j * 128:(j + 1) * 128]
            part[:, k * 128:(k + 1) * 128] = total

    for x, w, terms, span in ((x_img, w_img, lambda: d_img[...] + r_x[...], slice(0, n_img)),
                              (x_txt, w_txt, lambda: (d_txt[...] + r_p[...] + r_y[...]).T, slice(n_img, dw.shape[0]))):
        raw = jnp.dot(x[...], w[...], preferred_element_type=F32)
        inv = lax.rsqrt(jnp.sum(raw * raw, axis=1, keepdims=True))
        unit = raw * inv
        grad = scale[0] * terms()
        raw_grad = inv * (grad - unit * jnp.sum(unit * grad, axis=1, keepdims=True))
        dw[span, :] += lax.dot_general(x[...], raw_grad.astype(BF16), CONTRACT_ROWS, preferred_element_type=F32)


def weight_grads(scale, feat_img, feat_txt, w_img, w_txt, terms, sums):
    rows, blk = feat_img.shape[0], 512
    width = w_img.shape[1]
    n_all = feat_img.shape[1] + feat_txt.shape[1]
    by_row = lambda n: pl.BlockSpec((blk, n), lambda i: (i, 0))
    by_column = pl.BlockSpec((width, blk), lambda i: (0, i))
    whole = lambda shape: pl.BlockSpec(shape, lambda i: (0,) * len(shape))
    return pl.pallas_call(
        weight_kernel, name="weight_grads", grid=(rows // blk,),
        out_shape=(jax.ShapeDtypeStruct((n_all, width), F32), jax.ShapeDtypeStruct((8, 512), F32)),
        in_specs=[pl.BlockSpec(memory_space=pltpu.SMEM), by_row(feat_img.shape[1]), by_row(feat_txt.shape[1]),
                  whole(w_img.shape), whole(w_txt.shape), by_row(width), by_row(width), *[by_column] * 3, whole(sums.shape)],
        out_specs=(whole((n_all, width)), whole((8, 512))),
    )(scale, feat_img, feat_txt, w_img, w_txt, *terms, sums)


def reduce_kernel(x, part, out, total, acc, got, got_a, got_b, got_a2, got_b2, parts, send_sem, recv_sem, p_send, p_recv):
    me = lax.axis_index("data")
    core, cx, cy = me % 2, (me // 2) % 2, me // 4
    partner = flip_bits(core, cx, cy, 1, 0, 0)
    xn, yn = flip_bits(core, cx, cy, 0, 1, 0), flip_bits(core, cx, cy, 0, 0, 1)
    peers = [flip_bits(core, cx, cy, k % 2, (k // 2) % 2, k // 4) for k in range(1, 8)]
    enter(me, peers)
    half = x.shape[0] // 2
    quarter = half // 4
    eighth = quarter // 2

    def rows(start, size):
        return pl.ds(pl.multiple_of(start, 8), size)

    def copy(src, dst, k, to):
        return pltpu.make_async_remote_copy(src_ref=src, dst_ref=dst, send_sem=send_sem.at[k], recv_sem=recv_sem.at[k],
                                            device_id=(to,), device_id_type=MESH)

    def both(one, two):
        one.start()
        two.start()
        one.wait()
        two.wait()

    fold_halves = copy(x.at[rows((1 - core) * half, half)], got, 0, partner)
    fold_halves.start()
    part_copies = [
        pltpu.make_async_remote_copy(src_ref=part, dst_ref=parts.at[me], send_sem=p_send.at[k], recv_sem=p_recv.at[k],
                                     device_id=(peers[k],), device_id_type=MESH) for k in range(7)]
    for cp in part_copies:
        cp.start()
    parts[pl.ds(me, 1)] = part[...][None]
    fold_halves.wait()
    acc[...] = x[rows(core * half, half), :] + got[...]
    a1, b1 = cx * quarter, 2 * quarter + cy * quarter
    both(copy(acc.at[rows((1 - cx) * quarter, quarter)], got_a, 1, xn),
         copy(acc.at[rows(2 * quarter + (1 - cy) * quarter, quarter)], got_b, 2, yn))
    acc[rows(a1, quarter), :] += got_a[...]
    acc[rows(b1, quarter), :] += got_b[...]
    a2, b2 = a1 + cy * eighth, b1 + cx * eighth
    both(copy(acc.at[rows(a1 + (1 - cy) * eighth, eighth)], got_a2, 3, yn),
         copy(acc.at[rows(b1 + (1 - cx) * eighth, eighth)], got_b2, 4, xn))
    base = core * half
    out[rows(base + a2, eighth), :] = acc[rows(a2, eighth), :] + got_a2[...]
    out[rows(base + b2, eighth), :] = acc[rows(b2, eighth), :] + got_b2[...]

    def spread(start, size, k, to):
        span = rows(base + start, size)
        return copy(out.at[span], out.at[span], k, to)

    both(spread(a2, eighth, 5, yn), spread(b2, eighth, 6, xn))
    both(spread(a1, quarter, 7, xn), spread(b1, quarter, 8, yn))
    last = spread(0, half, 9, partner)
    last.start()
    for cp in part_copies:
        cp.wait()
    sum_parts = parts[0]
    for k in range(1, N_DEV):
        sum_parts = sum_parts + parts[k]
    total[...] = sum_parts
    last.wait()


def all_reduce(x, part):
    half, width = x.shape[0] // 2, x.shape[1]
    vmem = pl.BlockSpec(memory_space=pltpu.VMEM)
    buf = lambda n: pltpu.VMEM((n, width), F32)
    return pl.pallas_call(
        reduce_kernel, name="all_reduce",
        out_shape=(jax.ShapeDtypeStruct(x.shape, F32), jax.ShapeDtypeStruct(part.shape, F32)),
        in_specs=[vmem, vmem], out_specs=(vmem, vmem),
        scratch_shapes=[buf(half), buf(half), buf(half // 4), buf(half // 4), buf(half // 8), buf(half // 8),
                        pltpu.VMEM((N_DEV,) + part.shape, F32),
                        pltpu.SemaphoreType.DMA((10,)), pltpu.SemaphoreType.DMA((10,)),
                        pltpu.SemaphoreType.DMA((7,)), pltpu.SemaphoreType.DMA((7,))],
        compiler_params=pltpu.CompilerParams(collective_id=1, has_side_effects=True),
    )(x, part)


SEGMENTS = ((0, 0, 1, 0, 0), (4, 0, 1, 2, 0), (8, 4, 0, 0, 1), (12, 0, 1, 4, 0), (16, 5, 0, 0, 1), (20, 4, 1, 4, 0),
            (24, 4, 0, 5, 1), (27, 5, 0, 5, 1), (30, 0, 1, 5, 0), (34, 6, 1, 5, 0), (36, 0, 1, 6, 0), (40, 6, 1, 6, 0),
            (42, 6, 0, 0, 1), (46, 6, 0, 7, 0), (47, 7, 0, 0, 1), (51, 7, 0, 7, 0), (52, 0, 1, 7, 0), (56, 0, 1, 3, 0),
            (60, 0, 1, 1, 0))


def tile_at(t):
    code, last = 0, (0, 0)
    for first, i, di, j, dj in SEGMENTS:
        slope = 8 * di + dj
        line = (8 * i + j - slope * first, slope)
        step = (line[0] - last[0]) + (line[1] - last[1]) * t
        code = code + (step if first == 0 else lax.div(t + (64 - first), 64) * step)
        last = line
    return lax.div(code, 8), lax.rem(code, 8)


def pair_kernel(coef, emb_img, emb_txt, ids_sq, ids_half, ids_quarter, d_img, d_txt, r_x, r_p, r_y, sums,
                img, img_t, txt, di, dt, comb, ids_row, ids_col, ids_x, sb0, sb1, gb0, gb1, send_sem, recv_sem, own_sem):
    me = lax.axis_index("data")
    core, cx, cy = me % 2, (me // 2) % 2, me // 4
    flip = functools.partial(flip_bits, core, cx, cy)
    partner, xn, yn, yp = flip(1, 0, 0), flip(0, 1, 0), flip(0, 0, 1), flip(1, 0, 1)
    rows = emb_img.shape[0]
    q_rows = rows // 4
    enter(me, [partner, xn, yn, yp])

    def copy(k, src, dst, to):
        return pltpu.make_async_remote_copy(src_ref=src, dst_ref=dst, send_sem=send_sem.at[k], recv_sem=recv_sem.at[k],
                                            device_id=(to,), device_id_type=MESH)

    low, high = pl.ds(0, q_rows), pl.ds(q_rows, q_rows)

    def quarter(q):
        return pl.ds(q * q_rows, q_rows)

    feat_x = [copy(q, emb_img.at[quarter(q)], img.at[pl.ds(rows + q * q_rows, q_rows)], xn) for q in range(4)]
    feat_y = [copy(4 + q, emb_txt.at[quarter(q)], txt.at[4 + q, low], yn) for q in range(4)]
    feat_p = [copy(8 + h, emb_txt.at[pl.ds(h * COL_BLK, COL_BLK)], txt.at[2 + h], partner) for h in range(2)]
    pass_p = [copy(10 + q, txt.at[4 + q, low], txt.at[4 + q, high], partner) for q in range(4)]
    part_x = [copy(14 + q, di.at[pl.ds(rows + q * q_rows, q_rows)], r_x.at[quarter(q)], xn) for q in range(4)]
    part_c = [copy(18 + q, dt.at[4 + q, :, high], comb.at[q], partner) for q in range(4)]
    part_y = [copy(22 + q, dt.at[4 + q, :, low], r_y.at[:, quarter(q)], yn) for q in range(4)]
    part_p = [copy(26 + h, dt.at[2 + h], r_p.at[:, pl.ds(h * COL_BLK, COL_BLK)], partner) for h in range(2)]
    ids_p = copy(28, ids_half, ids_col.at[pl.ds(2, 2)], partner)
    ids_y = copy(29, ids_quarter, ids_col.at[pl.ds(4, 4), :, low], yn)
    ids_yp = copy(30, ids_quarter, ids_col.at[pl.ds(4, 4), :, high], yp)
    ids_xn = copy(31, ids_sq, ids_x.at[1], xn)
    every = [*feat_x, *feat_y, *feat_p, *pass_p, *part_x, *part_c, *part_y, *part_p, ids_p, ids_y, ids_yp, ids_xn]

    for cp in (ids_xn, ids_p, ids_y, ids_yp):
        cp.start()
    for q in range(4):
        feat_x[q].start()
        feat_y[q].start()
    for cp in feat_p:
        cp.start()
    own = [pltpu.make_async_copy(emb_img, img.at[pl.ds(0, rows)], own_sem.at[0]),
           pltpu.make_async_copy(emb_txt.at[pl.ds(0, COL_BLK)], txt.at[0], own_sem.at[1]),
           pltpu.make_async_copy(emb_txt.at[pl.ds(COL_BLK, COL_BLK)], txt.at[1], own_sem.at[2]),
           pltpu.make_async_copy(ids_half, ids_col.at[pl.ds(0, 2)], own_sem.at[3]),
           pltpu.make_async_copy(ids_sq, ids_x.at[0], own_sem.at[4])]
    for cp in own:
        cp.start()

    @pl.loop(0, 8)
    def _(k):
        di[pl.ds(pl.multiple_of(k * ROW_BLK, ROW_BLK), ROW_BLK), :] = jnp.zeros((ROW_BLK, di.shape[1]), F32)
        dt[k] = jnp.zeros(dt.shape[1:], F32)

    sums[...] = jnp.zeros_like(sums)
    gb1[...] = jnp.zeros_like(gb1)
    for cp in own:
        cp.wait()

    def spread_ids(which):
        columns = ids_x[which].T
        for k in range(rows // 128):
            ids_row[which * rows + k * 128:which * rows + (k + 1) * 128, :] = jnp.broadcast_to(
                columns[:, k:k + 1], (128, 128))

    def flip_rows(first, count):
        @pl.loop(first, first + count)
        def _(i):
            img_t[i] = img[pl.ds(pl.multiple_of(i * ROW_BLK, ROW_BLK), ROW_BLK), :].T

    spread_ids(0)
    flip_rows(0, 4)
    a, b = coef[0], coef[1]
    n_tiles = 64

    def row_span(i):
        return pl.ds(pl.multiple_of(i * ROW_BLK, ROW_BLK), ROW_BLK)

    def scores(sb, t):
        i, j = tile_at(t)
        sb[...] = lax.dot_general(img[row_span(i), :], txt[j], CONTRACT_COLS, preferred_element_type=F32)

    def gradients(gb, t):
        i, j = tile_at(t)
        di[row_span(i), :] += jnp.dot(gb[...], txt[j], preferred_element_type=F32)
        dt[j] += jnp.dot(img_t[i], gb[...], preferred_element_type=F32)

    def elementwise(sb, gb, t):
        i, j = tile_at(t)
        ids_c = ids_col[j]
        run, low_sum, gs_sum, g_sum = None, None, None, None
        for k in range(ROW_BLK // STRIP):
            s = sb[k * STRIP:(k + 1) * STRIP, :]
            ids_r = ids_row[pl.ds(i * ROW_BLK + k * STRIP, STRIP), 0:1]
            sign = jnp.where(ids_r == ids_c, -1.0, 1.0).astype(F32)
            neg = (s * a + b) * sign
            w = jnp.exp2(-jnp.abs(neg))
            d = 1.0 + w
            g = sign / (1.0 + jnp.exp2(neg))
            low_k, gs = jnp.minimum(neg, 0.0), g * s
            for u in range(STRIP // 8):
                at8 = slice(u * 8, u * 8 + 8)
                run = w[at8] if run is None else run * d[at8] + w[at8]
                low_sum = low_k[at8] if low_sum is None else low_sum + low_k[at8]
                gs_sum = gs[at8] if gs_sum is None else gs_sum + gs[at8]
                g_sum = g[at8] if g_sum is None else g_sum + g[at8]
            gb[k * STRIP:(k + 1) * STRIP, :] = g.astype(BF16)
        sums[0] += low_sum
        sums[1] += jnp.log1p(run)
        sums[2] += gs_sum
        sums[3] += g_sum

    def join(q):
        part_c[q].wait_recv()
        dt[4 + q, :, 0:q_rows] += comb[q]
        part_y[q].start()

    def x_rows():
        spread_ids(1)
        flip_rows(4, 1)

    scores(sb0, 0)

    @pl.loop(0, n_tiles // 2)
    def _(f):
        def on(at, arrivals=(), starts=(), then=None):
            @pl.when(f == at)
            def _():
                for cp in arrivals:
                    cp.wait_recv()
                for cp in starts:
                    cp.start()
                if then is not None:
                    then()

        on(1, [*feat_p, ids_p])
        on(3, [feat_x[0], ids_xn], then=x_rows)
        on(4, [feat_y[0], ids_y, ids_yp], [pass_p[0]])
        on(5, [pass_p[0]])
        on(6, [feat_y[1]], [pass_p[1]])
        on(7, [feat_x[1]], then=functools.partial(flip_rows, 5, 1))
        on(8, [feat_y[2]], [pass_p[2]])
        on(10, [feat_x[2]], then=functools.partial(flip_rows, 6, 1))
        on(11, [feat_x[3], feat_y[3], pass_p[1]], [pass_p[3]], then=functools.partial(flip_rows, 7, 1))
        on(12, [pass_p[2], pass_p[3]])
        on(13, (), [part_c[0]])
        on(14, (), [part_x[0]], then=functools.partial(join, 0))
        on(16, (), [part_x[1]])
        on(19, (), [part_c[1]])
        on(20, then=functools.partial(join, 1))
        on(22, (), [part_c[2]])
        on(23, then=functools.partial(join, 2))
        on(24, (), [part_x[2]])
        on(26, (), [part_p[0]])
        on(27, (), [part_x[3]])
        on(29, (), [part_c[3]])
        on(30, then=functools.partial(join, 3))
        on(31, (), [part_p[1]])

        t = 2 * f
        scores(sb1, t + 1)
        elementwise(sb0, gb0, t)
        gradients(gb1, jnp.maximum(t - 1, 0))
        scores(sb0, lax.rem(t + 2, n_tiles))
        elementwise(sb1, gb1, t + 1)
        gradients(gb0, t)

    gradients(gb1, n_tiles - 1)
    outs = [pltpu.make_async_copy(di.at[pl.ds(0, rows)], d_img, own_sem.at[0]),
            pltpu.make_async_copy(dt.at[0], d_txt.at[:, pl.ds(0, COL_BLK)], own_sem.at[1]),
            pltpu.make_async_copy(dt.at[1], d_txt.at[:, pl.ds(COL_BLK, COL_BLK)], own_sem.at[2])]
    for cp in outs:
        cp.start()
    for cp in outs:
        cp.wait()
    for cp in (*part_x, *part_p, *part_y):
        cp.wait_recv()
    for cp in every:
        cp.wait_send()


def pair_grads(coef, emb_img, emb_txt, ids):
    rows, width = emb_img.shape
    hbm = pl.BlockSpec(memory_space=pl.ANY)
    vmem = pl.BlockSpec(memory_space=pltpu.VMEM)
    grads, grads_t = jax.ShapeDtypeStruct((rows, width), F32), jax.ShapeDtypeStruct((width, rows), F32)
    return pl.pallas_call(
        pair_kernel,
        name="pair_grads",
        out_shape=(grads, grads_t, grads, grads_t, grads_t, jax.ShapeDtypeStruct((4, 8, COL_BLK), F32)),
        in_specs=[pl.BlockSpec(memory_space=pltpu.SMEM), hbm, hbm, hbm, hbm, hbm],
        out_specs=(hbm, hbm, hbm, hbm, hbm, vmem),
        scratch_shapes=[
            pltpu.VMEM((2 * rows, width), BF16),
            pltpu.VMEM((8, width, ROW_BLK), BF16),
            pltpu.VMEM((8, COL_BLK, width), BF16),
            pltpu.VMEM((2 * rows, width), F32),
            pltpu.VMEM((8, width, COL_BLK), F32),
            pltpu.VMEM((4, width, rows // 4), F32),
            pltpu.VMEM((2 * rows, 128), jnp.int32),
            pltpu.VMEM((8, 1, COL_BLK), jnp.int32),
            pltpu.VMEM((2, rows // 128, 128), jnp.int32),
            pltpu.VMEM((ROW_BLK, COL_BLK), F32),
            pltpu.VMEM((ROW_BLK, COL_BLK), F32),
            pltpu.VMEM((ROW_BLK, COL_BLK), BF16),
            pltpu.VMEM((ROW_BLK, COL_BLK), BF16),
            pltpu.SemaphoreType.DMA((32,)),
            pltpu.SemaphoreType.DMA((32,)),
            pltpu.SemaphoreType.DMA((5,)),
        ],
        compiler_params=pltpu.CompilerParams(collective_id=0, has_side_effects=True, vmem_limit_bytes=67_000_000),
    )(coef, emb_img, emb_txt, ids.reshape(rows // 128, 128), ids.reshape(2, 1, COL_BLK), ids.reshape(4, 1, rows // 4))


def solution(mesh):
    n_dev = mesh.shape["data"]

    def local_fn(feat_img, feat_txt, w_img, w_txt, log_temp, logit_bias, pair_ids):
        total_rows = feat_img.shape[0] * n_dev
        temp_scale = jnp.exp(log_temp)
        emb_img, emb_txt = embed(feat_img, feat_txt, w_img, w_txt)
        coef = jnp.stack([-LOG2E * temp_scale, -LOG2E * logit_bias])
        d_img, d_txt, r_x, r_p, r_y, sums = pair_grads(coef, emb_img, emb_txt, pair_ids)
        scale = temp_scale / total_rows
        dw, part = weight_grads(scale[None], feat_img, feat_txt, w_img, w_txt, (d_img, r_x, d_txt, r_p, r_y), sums)
        dw, total = all_reduce(dw, part)
        total = jnp.sum(total.reshape(8, 4, 128), axis=(0, 2))
        n_img = feat_img.shape[1]
        loss = (total[1] - total[0] / LOG2E) / total_rows
        return loss, scale * total[2], total[3] / total_rows, dw[:n_img], dw[n_img:]

    return jax.shard_map(
        local_fn,
        mesh=mesh,
        in_specs=(P("data", None), P("data", None), P(None, None), P(None, None), P(), P(), P("data")),
        out_specs=(P(), P(), P(), P(None, None), P(None, None)),
        check_vma=False,
    )
```
